32 devices in a mesh: section: 4 (over y, core), wide: 2 (over x), narrow: 4 (over z).
Axes of the slice: x: 2, y: 2, z: 4, core: 2. Of those that a mesh axis runs over, the one named last changes fastest.
Arguments:
- normed_inputs: bfloat16 [4, 4, 4, 192, 4096], P('section', 'narrow', None, 'wide'), may hold values from -160 to 160
- value_cotangent: bfloat16 [4, 4, 4, 192, 1024], P('section', 'narrow', None, 'wide'), may hold values from -6 to 6
- expert_hidden: bfloat16 [4, 4, 4, 64, 7168], P('section', 'narrow', None, None, 'wide'), may hold values from -40 to 40
- expert_cotangent: bfloat16 [4, 4, 4, 64, 4096], P('section', 'narrow', None, 'wide'), may hold values from -110 to 110
- slot_gate: bfloat16 [4, 4, 4, 64], P('section', 'narrow', None, 'wide'), may hold values from 0.25 to 1
- slot_count: int32 [4, 4, 4], P('section', 'narrow'), may hold values from 33 to 64, as said below
- expert_weight: bfloat16 [4, 7168, 4096], P('section', 'wide', 'narrow'), may hold values from -0.0625 to 0.0625
- expert_moment: float32 [4, 7168, 4096], P('section', 'wide', 'narrow'), may hold values from -6 to 6
- value_weight: bfloat16 [4, 4096, 1024], P('section', ('wide', 'narrow')), may hold values from -0.09375 to 0.09375
- value_moment: float32 [4, 4096, 1024], P('section', ('wide', 'narrow')), may hold values from -6 to 6
Outputs:
- expert_weight_next: bfloat16 [4, 7168, 4096], P('section', 'wide', 'narrow')
- expert_moment_next: float32 [4, 7168, 4096], P('section', 'wide', 'narrow')
- value_weight_next: bfloat16 [4, 4096, 1024], P('section', ('wide', 'narrow'))
- value_moment_next: float32 [4, 4096, 1024], P('section', ('wide', 'narrow'))
The draws below stay inside these ranges and needn't reach their ends.
Inputs may be any that keep to these rules, and one draw needn't show every extreme that they name: The live slots of a micro-batch are slots 0 to slot_count - 1; in every layer and replica some micro-batch fills all 64 slots.
All inputs are finite; a program needn't handle non-finite values.
Results may differ from the reference program's by a relative error of at most 0.014.
Values may be sent and summed in bfloat16 or wider, within the bound.
A program may use at most 192 MiB of HBM per device.

```python
import math
import jax
import jax.numpy as jnp
from jax import lax

D = 4096
FF = 7168
KV = 1024
MICRO = 4
MB_DEV = 96
SECTIONS = 4
REPLICAS = 4
SEQ = 192
SLOTS = 64
N_WIDE = 2


def rough_field(base_key, extent, section_rise, divisor):
    subkeys = jax.random.split(base_key, 3)
    columns = extent[-1]
    layers = extent[0]
    column_pos = jnp.arange(columns, dtype=jnp.float32) / max(columns - 1, 1)
    column_scale = jnp.exp(math.log(3.0) * column_pos + jax.random.uniform(subkeys[0], (columns,), jnp.float32, 0.0, math.log(3.3)))
    layer_pos = jnp.arange(layers, dtype=jnp.float32) / max(layers - 1, 1)
    layer_scale = jnp.exp(section_rise * math.log(3.0) * layer_pos).reshape(layers, 1, 1, 1, 1)
    row_scale = jnp.exp(jax.random.uniform(subkeys[1], extent[:-1] + (1,), jnp.float32, 0.0, math.log(3.0)))
    values = jnp.clip(jax.random.normal(subkeys[2], extent, jnp.float32), -6.0, 6.0)
    return values * row_scale * column_scale * layer_scale / divisor


def draw_normed_inputs(key, part):
    return rough_field(jax.random.fold_in(key, 3), (SECTIONS, REPLICAS, MICRO, SEQ, D), 1.0, 4.0).astype(jnp.bfloat16)


def draw_expert_hidden(key, part):
    return rough_field(jax.random.fold_in(key, 5), (SECTIONS, REPLICAS, MICRO, SLOTS, FF), 0.0, 6.0).astype(jnp.bfloat16)


def draw_expert_cotangent(key, part):
    return rough_field(jax.random.fold_in(key, 7), (SECTIONS, REPLICAS, MICRO, SLOTS, D), 1.0, 6.0).astype(jnp.bfloat16)


def draw_slot_count(key, part):
    count_key = jax.random.fold_in(key, 11)
    pick_key = jax.random.fold_in(key, 13)
    counts = jax.random.randint(count_key, (SECTIONS, REPLICAS, MICRO), SLOTS // 2 + 1, SLOTS + 1, dtype=jnp.int32)
    chosen = jax.random.randint(pick_key, (SECTIONS, REPLICAS, 1), 0, MICRO, dtype=jnp.int32)
    positions = jnp.arange(MICRO, dtype=jnp.int32).reshape(1, 1, MICRO)
    return jnp.where(positions == chosen, jnp.int32(SLOTS), counts).astype(jnp.int32)


def block_scale(key, dims, cuts, smallest, high):
    level = 1.0
    for position, parts in cuts:
        heights = jax.random.uniform(jax.random.fold_in(jax.random.fold_in(key, 6), position), (parts,), jnp.float32, smallest / len(cuts), high / len(cuts))
        level = level * jnp.repeat(jnp.exp(heights), dims[position] // parts).reshape((-1,) + (1,) * (len(dims) - 1 - position))
    return level


def scatter_about(key, shape, deviation, reach, shards=(), held_as=jnp.bfloat16):
    level = block_scale(key, shape, shards, -0.22, 0.18) if shards else 1.0
    entries = jax.random.normal(key, shape, jnp.float32) * deviation * level
    return jnp.minimum(jnp.maximum(entries, -reach), reach).astype(held_as)


def setup_inputs(seed: int = 0) -> dict:
    key_of = jax.random.split(jax.random.key(seed), 11)
    normed_inputs = draw_normed_inputs(jax.random.fold_in(key_of[10], 71), 0)
    value_cotangent = scatter_about(key_of[1], (SECTIONS, REPLICAS, MICRO, SEQ, KV), 1.0, 6.0, ((0, 4), (1, 4), (3, 2)))
    expert_hidden = draw_expert_hidden(jax.random.fold_in(key_of[10], 71), 0)
    expert_cotangent = draw_expert_cotangent(jax.random.fold_in(key_of[10], 71), 0)
    slot_gate = jnp.clip(0.25 + 0.75 * jax.random.uniform(key_of[4], (SECTIONS, REPLICAS, MICRO, SLOTS), jnp.float32) ** block_scale(key_of[4], (SECTIONS, REPLICAS, MICRO, SLOTS), ((0, 4), (1, 4), (3, 2)), -0.2, 0.2), 0.25, 1.0).astype(jnp.bfloat16)
    slot_count = draw_slot_count(jax.random.fold_in(key_of[10], 71), 0)
    expert_weight = scatter_about(key_of[6], (SECTIONS, FF, D), FF ** -0.5, 0.0625, ((0, 4), (1, 2), (2, 4)))
    expert_moment = scatter_about(key_of[7], (SECTIONS, FF, D), 1.0, 6.0, ((0, 4), (1, 2), (2, 4)), jnp.float32)
    value_weight = scatter_about(key_of[8], (SECTIONS, D, KV), D ** -0.5, 0.09375, ((0, 4), (1, 8)))
    value_moment = scatter_about(key_of[9], (SECTIONS, D, KV), 1.0, 6.0, ((0, 4), (1, 8)), jnp.float32)
    return {"normed_inputs": normed_inputs, "value_cotangent": value_cotangent, "expert_hidden": expert_hidden, "expert_cotangent": expert_cotangent, "slot_gate": slot_gate, "slot_count": slot_count, "expert_weight": expert_weight, "expert_moment": expert_moment, "value_weight": value_weight, "value_moment": value_moment}


MOMENTUM_DECAY = 0.9
STEP_RATE = 0.01

def rounded_add(accumulated, product):
    kept = lax.optimization_barrier(product.astype(jnp.bfloat16))
    return accumulated + kept.astype(jnp.float32)

def expert_layer(hidden_layer, cotangent_layer, gate_layer, count_layer):
    positions = jnp.arange(SLOTS, dtype=jnp.int32)
    live = positions[None, None, :] < count_layer[:, :, None]
    coefficient = jnp.where(live, gate_layer.astype(jnp.float32), jnp.zeros(gate_layer.shape, jnp.float32))
    scaled = (coefficient[..., None] * cotangent_layer.astype(jnp.float32)).astype(jnp.bfloat16)

    def add_replica(accumulated, pieces):
        hidden_rows = pieces[0].reshape(-1, FF)
        scaled_rows = pieces[1].reshape(-1, D)
        product = jnp.dot(hidden_rows.T, scaled_rows, preferred_element_type=jnp.float32)
        return (rounded_add(accumulated, product), None)
    result, ignored = lax.scan(add_replica, jnp.zeros((FF, D), jnp.float32), (hidden_layer, scaled))
    return result

def value_layer(input_layer, cotangent_layer):
    device_inputs = input_layer.reshape(REPLICAS, MICRO, N_WIDE, MB_DEV, D).transpose(0, 2, 1, 3, 4).reshape(REPLICAS * N_WIDE, MICRO * MB_DEV, D)
    device_cotangents = cotangent_layer.reshape(REPLICAS, MICRO, N_WIDE, MB_DEV, KV).transpose(0, 2, 1, 3, 4).reshape(REPLICAS * N_WIDE, MICRO * MB_DEV, KV)

    def add_device(accumulated, pieces):
        product = jnp.dot(pieces[0].T, pieces[1], preferred_element_type=jnp.float32)
        return (rounded_add(accumulated, product), None)
    result, ignored = lax.scan(add_device, jnp.zeros((D, KV), jnp.float32), (device_inputs, device_cotangents))
    return result

def reference(normed_inputs, value_cotangent, expert_hidden, expert_cotangent, slot_gate, slot_count, expert_weight, expert_moment, value_weight, value_moment):
    expert_grads = []
    value_grads = []
    for layer_index in range(SECTIONS):
        expert_grads.append(expert_layer(expert_hidden[layer_index], expert_cotangent[layer_index], slot_gate[layer_index], slot_count[layer_index]))
        value_grads.append(value_layer(normed_inputs[layer_index], value_cotangent[layer_index]))
    expert_grad = jnp.stack(expert_grads)
    value_grad = jnp.stack(value_grads)
    overall = jnp.sum(expert_grad * expert_grad) + jnp.sum(value_grad * value_grad)
    entry_count = SECTIONS * (FF * D + D * KV)
    factor = jnp.minimum(1.0, math.sqrt(entry_count) / jnp.sqrt(overall + 1e-06))
    expert_next = MOMENTUM_DECAY * expert_moment + factor * expert_grad
    value_next = MOMENTUM_DECAY * value_moment + factor * value_grad
    expert_weight_next = (expert_weight.astype(jnp.float32) - STEP_RATE * expert_next).astype(jnp.bfloat16)
    value_weight_next = (value_weight.astype(jnp.float32) - STEP_RATE * value_next).astype(jnp.bfloat16)
    return (expert_weight_next, expert_next, value_weight_next, value_next)
```

```python
import math

import jax
import jax.numpy as jnp
from jax import lax
from jax.sharding import PartitionSpec as P

MOMENTUM_DECAY = 0.9
STEP_RATE = 0.01


def shifted(x, axis, k):
    n = lax.axis_size(axis)
    return lax.ppermute(x, axis, [(i, (i + k) % n) for i in range(n)])


def hop(x, axis, first, direction):
    n = lax.axis_size(axis)
    pairs = [(i, i + 1) for i in range(first, n - 1)]
    if direction < 0:
        pairs = [(n - 1 - i, n - 1 - j) for i, j in pairs]
    return lax.ppermute(x, axis, pairs)


def chunk(x, axis, k, dim):
    n = lax.axis_size(axis)
    size = x.shape[dim] // n
    owner = lax.rem(lax.axis_index(axis) + k, n)
    return lax.dynamic_slice_in_dim(x, owner * size, size, dim)


def on_device(
    normed_inputs,
    value_cotangent,
    expert_hidden,
    expert_cotangent,
    slot_gate,
    slot_count,
    expert_weight,
    expert_moment,
    value_weight,
    value_moment,
):
    n_wide = lax.axis_size("wide")
    n_narrow = lax.axis_size("narrow")
    wide_index = lax.axis_index("wide")
    narrow_index = lax.axis_index("narrow")
    input_rows = normed_inputs[0, 0].reshape(-1, normed_inputs.shape[-1])
    value_cot_rows = value_cotangent[0, 0].reshape(-1, value_cotangent.shape[-1])
    hidden = expert_hidden[0, 0]
    cotangent = expert_cotangent[0, 0]
    micro, slots, _ = cotangent.shape

    positions = wide_index * slots + jnp.arange(slots, dtype=jnp.int32)
    live = positions[None, :] < slot_count[0, 0][:, None]
    coefficient = jnp.where(live, slot_gate[0, 0].astype(jnp.float32), 0.0)
    scaled = (coefficient[:, :, None] * cotangent.astype(jnp.float32)).astype(jnp.bfloat16)

    columns = [chunk(scaled, "narrow", 0, 2)]
    for k in range(1, n_narrow):
        columns.append(shifted(chunk(scaled, "narrow", k, 2), "narrow", k))

    up = [hidden]
    down = [hidden]
    for k in range(1, n_narrow):
        up.append(hop(up[-1], "narrow", k - 1, 1))
        down.append(hop(down[-1], "narrow", k - 1, -1))
    hiddens = [hidden] + [
        jnp.where(narrow_index >= k, up[k], down[n_narrow - k]) for k in range(1, n_narrow)
    ]

    rows_in = [chunk(input_rows, "wide", 0, 1)]
    cots_in = [value_cot_rows]
    for k in range(1, n_wide):
        rows_in.append(shifted(chunk(input_rows, "wide", k, 1), "wide", k))
        cots_in.append(shifted(value_cot_rows, "wide", k))
    rows_in, up[1], down[1] = lax.optimization_barrier((rows_in, up[1], down[1]))
    value_part = lax.dot_general(
        jnp.concatenate(rows_in, 0),
        jnp.concatenate(cots_in, 0),
        (((0,), (0,)), ((), ())),
        preferred_element_type=jnp.float32,
    ).astype(jnp.bfloat16)
    stacked, value_part = lax.optimization_barrier((jnp.stack(columns), value_part))
    width = stacked.shape[-1]
    gathered = jnp.zeros((n_narrow, micro, n_wide, slots, width), jnp.bfloat16)
    for k in range(n_wide):
        piece = stacked if k == 0 else shifted(stacked, "wide", k)
        source = lax.rem(wide_index + n_wide - k, n_wide)
        gathered = lax.dynamic_update_slice(gathered, piece[:, :, None], (0, 0, source, 0, 0))
    gathered = gathered.reshape(n_narrow, micro, n_wide * slots, width)

    above = below = None
    for step in range(1, n_narrow):
        far = n_narrow - step
        senders = range(step)
        to_up = chunk(value_part, "narrow", far, 0)
        to_down = chunk(value_part, "narrow", step, 0)
        if above is not None:
            to_up = (to_up.astype(jnp.float32) + above.astype(jnp.float32)).astype(jnp.bfloat16)
            to_down = (to_down.astype(jnp.float32) + below.astype(jnp.float32)).astype(jnp.bfloat16)
        above = lax.ppermute(to_up, "narrow", [(i, i + 1) for i in senders])
        below = lax.ppermute(
            to_down, "narrow", [(n_narrow - 1 - i, n_narrow - 2 - i) for i in senders]
        )
    value_grad = (
        chunk(value_part, "narrow", 0, 0).astype(jnp.float32)
        + above.astype(jnp.float32)
        + below.astype(jnp.float32)
    )

    left = jnp.stack(hiddens).reshape(-1, hidden.shape[-1])
    right = gathered.reshape(-1, width)
    expert_grad = lax.dot_general(
        left, right, (((0,), (0,)), ((), ())), preferred_element_type=jnp.float32
    )

    squares = jnp.sum(expert_grad * expert_grad) + jnp.sum(value_grad * value_grad)
    overall = lax.psum(squares, ("section", "wide", "narrow"))
    layer_entries = expert_grad.size + value_grad.size
    entry_count = lax.axis_size("section") * n_wide * n_narrow * layer_entries
    factor = jnp.minimum(1.0, math.sqrt(entry_count) / jnp.sqrt(overall + 1e-06))
    expert_next = MOMENTUM_DECAY * expert_moment[0] + factor * expert_grad
    value_next = MOMENTUM_DECAY * value_moment[0] + factor * value_grad
    expert_weight_next = (expert_weight[0].astype(jnp.float32) - STEP_RATE * expert_next).astype(
        jnp.bfloat16
    )
    value_weight_next = (value_weight[0].astype(jnp.float32) - STEP_RATE * value_next).astype(
        jnp.bfloat16
    )
    return (expert_weight_next[None], expert_next[None], value_weight_next[None], value_next[None])


def solution(mesh):
    return jax.shard_map(
        on_device,
        mesh=mesh,
        in_specs=(
            P("section", "narrow", None, "wide", None),
            P("section", "narrow", None, "wide", None),
            P("section", "narrow", None, None, "wide"),
            P("section", "narrow", None, "wide", None),
            P("section", "narrow", None, "wide"),
            P("section", "narrow", None),
            P("section", "wide", "narrow"),
            P("section", "wide", "narrow"),
            P("section", ("wide", "narrow"), None),
            P("section", ("wide", "narrow"), None),
        ),
        out_specs=(
            P("section", "wide", "narrow"),
            P("section", "wide", "narrow"),
            P("section", ("wide", "narrow"), None),
            P("section", ("wide", "narrow"), None),
        ),
        check_vma=False,
    )
```
